32 devices in a mesh: tok: 8 (over z, y), vocab: 4 (over x, core).
Axes of the slice: x: 2, y: 2, z: 4, core: 2. Of those that a mesh axis runs over, the one named last changes fastest.
Arguments:
- hidden: bfloat16 [192, 9216], P('tok'), may hold values from -256 to 256
- policy_head: bfloat16 [9216, 32768], P(None, ('tok', 'vocab')), may hold values from -0.0625 to 0.0625
- reference_head: bfloat16 [9216, 32768], P(None, ('tok', 'vocab')), may hold values from -0.0625 to 0.0625
- targets: int32 [192], P('tok'), may hold values from 0 to 32767
Outputs:
- policy_logprob: float32 [192], P('tok')
- reference_logprob: float32 [192], P('tok')
- divergence: float32 [192], P('tok')
The draws below stay inside these ranges and needn't reach their ends.
All inputs are finite; a program needn't handle non-finite values.
Results may differ from the reference program's by a relative error of at most 0.00055.
Values may be sent and summed in bfloat16 or wider, within the bound.
No kernel may reach another device: no remote copies, remote signals or barrier semaphores. Data moves between devices by JAX's collectives and lax.ppermute only.
A program may use at most 128 MiB of HBM per device.

```python
import math
import jax
import jax.numpy as jnp
import numpy as np

D = 9216
TOKENS = 192
V = 32768


def draw_hidden(key, part):
    key_base, key_scale = jax.random.split(key, 2)
    base = jax.random.normal(key_base, (TOKENS, D), jnp.float32)
    base = jnp.clip(base, -6.0, 6.0)
    scales = jnp.exp(jax.random.uniform(key_scale, (TOKENS, 1), jnp.float32, 0.0, math.log(4.0)))
    return (base * scales).astype(jnp.bfloat16)


def plant(entries, rng, smallest, top_value):
    longest = entries.shape.index(max(entries.shape))
    spots = []
    for shift in (0, 1):
        where = [jax.random.randint(jax.random.fold_in(rng, axis), (), 0, length) for axis, length in enumerate(entries.shape)]
        where[longest] = (where[longest] + shift) % entries.shape[longest]
        spots.append(tuple(where))
    return entries.at[spots[0]].set(smallest).at[spots[1]].set(top_value)


def block_levels(own_key, dims, cuts, smallest, top_value):
    gain = 1.0
    for position, blocks in cuts:
        steps = jax.random.uniform(jax.random.fold_in(jax.random.fold_in(own_key, 6), position), (blocks,), jnp.float32, smallest / len(cuts), top_value / len(cuts))
        gain = gain * jnp.repeat(jnp.exp(steps), dims[position] // blocks).reshape((-1,) + (1,) * (len(dims) - 1 - position))
    return gain


def rank_table(amount, slope):
    loads = [(1 << 20) // math.isqrt(standing ** slope) + 1 for standing in range(1, amount + 1)]
    scale = 1 + sum(loads) // (1 << 30)
    return np.cumsum(np.array([max(1, weight // scale) for weight in loads]))


def ranked_ids(key, dims, number_of, slope):
    table = rank_table(number_of, slope)
    ticket = jax.random.randint(jax.random.fold_in(key, 1), dims, 0, int(table[number_of - 1]))
    grade = jnp.searchsorted(jnp.asarray(table, jnp.int32), ticket, side="right")
    return jax.random.permutation(jax.random.fold_in(key, 2), number_of)[grade].astype(jnp.int32)


def scatter_about(stream_key, extent, spread, reach, pieces=(), kind=jnp.bfloat16):
    result = jax.random.normal(stream_key, extent, jnp.float32) * spread
    if len(pieces) > 0:
        result = block_levels(stream_key, extent, pieces, -0.22, 0.18) * result
    return jnp.clip(result, min=-reach, max=reach).astype(kind)


def setup_inputs(seed: int = 0) -> dict:
    splits = jax.random.split(jax.random.key(seed), 5)
    return {
        "hidden": draw_hidden(jax.random.fold_in(splits[4], 71), 0),
        "policy_head": scatter_about(splits[1], (D, V), D ** -0.5, 0.0625, ((1, 32),)),
        "reference_head": scatter_about(splits[2], (D, V), D ** -0.5, 0.0625, ((1, 32),)),
        "targets": plant(ranked_ids(splits[3], (TOKENS,), V, 2), jax.random.fold_in(splits[3], 3), 0, V - 1).astype(jnp.int32),
    }


def reference(hidden, policy_head, reference_head, targets):
    policy_logits = jnp.dot(hidden, policy_head, preferred_element_type=jnp.float32)
    reference_logits = jnp.dot(hidden, reference_head, preferred_element_type=jnp.float32)
    peak_policy = jnp.max(policy_logits, axis=1)
    peak_reference = jnp.max(reference_logits, axis=1)
    policy_exp = jnp.exp(policy_logits - peak_policy[:, None])
    total_policy = jnp.sum(policy_exp, axis=1)
    total_reference = jnp.sum(jnp.exp(reference_logits - peak_reference[:, None]), axis=1)
    weighted = jnp.sum(policy_exp * (policy_logits - reference_logits), axis=1)
    vocab_ids = jnp.arange(policy_logits.shape[1], dtype=jnp.int32)
    target_hits = vocab_ids[None, :] == targets.astype(jnp.int32)[:, None]
    target_policy = jnp.sum(jnp.where(target_hits, policy_logits, jnp.zeros_like(policy_logits)), axis=1)
    target_reference = jnp.sum(jnp.where(target_hits, reference_logits, jnp.zeros_like(reference_logits)), axis=1)
    log_norm_policy = peak_policy + jnp.log(total_policy)
    log_norm_reference = peak_reference + jnp.log(total_reference)
    policy_logprob = target_policy - log_norm_policy
    reference_logprob = target_reference - log_norm_reference
    divergence = weighted / total_policy - log_norm_policy + log_norm_reference
    return (policy_logprob, reference_logprob, divergence)
```

```python
import functools

import jax
import jax.numpy as jnp
from jax import lax
from jax.experimental import pallas as pl
from jax.experimental.pallas import tpu as pltpu
from jax.sharding import PartitionSpec as P


LANES = 128
TILE = 512
CHUNK = 768
STATS = 7
SPLIT = 9216
AHEAD = 0
MARGIN = 4 << 20


def hop(value, mask, count):
    pairs = [(i, i ^ mask) for i in range(count)]
    return lax.ppermute(value, ("tok", "vocab"), pairs)


def with_ids(columns, targets):
    digits = jnp.stack([(targets >> (8 * k)) & 255 for k in range(3)], axis=1)
    digits = jnp.pad(digits, ((0, 0), (0, LANES - 3)))
    return jnp.concatenate(columns + [digits.astype(columns[0].dtype)], axis=1)


class Plan:
    def __init__(self, depth, vocab_count):
        unit = vocab_count * LANES
        self.wide = min(SPLIT, depth) // unit * unit // vocab_count
        self.rest = depth - self.wide * vocab_count
        self.both = self.rest // 2
        self.vocab_count = vocab_count

    def starts(self, v):
        return v * self.wide, self.wide * self.vocab_count + (v & 1) * self.both

    def spans(self, near):
        found = []
        for m in range(self.vocab_count):
            if (m < 2) == near:
                found.append((m, 0, self.wide, 0))
                if m < 2 and self.both:
                    found.append((m, self.wide, self.both, 1))
        return found


def sends(tok_count):
    if tok_count == 8:
        return [[1, 2], [4], [6, 3, 5], [7]]
    return [list(range(1, tok_count))]


def turns(tok_count):
    if tok_count == 8:
        return [[1, 2, 4, 3], [6, 5, 7]]
    return [list(range(1, tok_count))]


def gather_rows(hidden, targets, plan, tok_count, vocab_count):
    rows = hidden.shape[0]
    me = lax.axis_index("vocab")

    def move(value, mask):
        return hop(value, mask, tok_count * vocab_count)

    def own(v, full):
        one, two = plan.starts(v)
        parts = [lax.dynamic_slice_in_dim(hidden, one, plan.wide, axis=1)]
        if full and plan.both:
            parts.append(lax.dynamic_slice_in_dim(hidden, two, plan.both, axis=1))
        return parts

    first = with_ids(own(me, True), targets)
    along, across = {0: first}, {}
    step = tok_count // 4
    while step >= 1:
        along.update({k ^ step: move(along[k], step * 2 * vocab_count) for k in list(along)})
        step //= 2
    for k in along:
        across[k] = move(along[k], vocab_count)
    blocks = {2 * k: along[k] for k in along} | {2 * k + 1: across[k] for k in across}
    pieces = {0: [(blocks[b], 0, b) for b in blocks]}

    def joined(names, width):
        return jnp.concatenate([blocks[b][:, :width] for b in names], axis=0)

    for m in range(vocab_count):
        if m % 2:
            continue
        if m:
            pieces[m] = [(own(me ^ m, False)[0], 0, 0)]
            for names in sends(tok_count):
                got = move(joined(names, plan.wide), m)
                pieces[m] += [(got, i * rows, b) for i, b in enumerate(names)]
        pieces[m + 1] = [(jnp.concatenate(own(me ^ (m + 1), m == 0), axis=1), 0, 0)]
        if m == 0:
            groups = [(joined(names, plan.wide + plan.both), [(i * rows, b) for i, b in enumerate(names)]) for names in turns(tok_count)]
        else:
            seen = {}
            for array, at, b in pieces[m][1:]:
                seen.setdefault(id(array), (array, []))[1].append((at, b))
            groups = list(seen.values())
        for array, places in groups:
            got = move(array, 1)
            pieces[m + 1] += [(got, at, b) for at, b in places]
    return pieces


def chunked(spans):
    found, at = [], 0
    for m, _, width, kind in spans:
        for cut in range(0, width, CHUNK):
            part = min(CHUNK, width - cut)
            found.append((at, (m, kind), cut, part))
            at += part
    return found


def copies_of(cut_spans, plan, heads, stores, sems, low):
    found = []
    me = lax.axis_index("vocab")
    for i, (at, key, cut, part) in enumerate(cut_spans):
        for j, (head, store) in enumerate(zip(heads, stores)):
            start = plan.starts(me ^ key[0])[key[1]]
            src = pl.ds(pl.multiple_of(start, LANES) + cut, part)
            found.append(pltpu.make_async_copy(head.at[src, :], store.at[pl.ds(at - low, part), :], sems.at[i, j]))
    return found


def load_kernel(cuts, plan, policy_ref, reference_ref, stored, sems):
    copies = copies_of(cuts, plan, (policy_ref, reference_ref), [stored.at[0], stored.at[1]], sems, 0)
    for copy in copies:
        copy.start()
    for copy in copies:
        copy.wait()


def fill(layout, refs, rows, lhs):
    for index, row, column, width, block, to in layout:
        lhs[block * rows : (block + 1) * rows, to : to + width] = refs[index][row : row + rows, column : column + width]


def multiply(lhs, low, high, store, tile, put):
    @pl.loop(0, store.shape[1] // tile)
    def _(step):
        at = pl.ds(pl.multiple_of(step * tile, tile), tile)
        put(at, jnp.dot(lhs[:, low:high], store[0 : high - low, at], preferred_element_type=jnp.float32))


def partial_kernel(layout, count, rows, tile, *refs):
    blocks, stored, outs, lhs = refs[:count], refs[count], refs[count + 1 : count + 3], refs[count + 3]
    fill(layout, blocks, rows, lhs)
    for j, out in enumerate(outs):

        def put(at, value):
            out[:, at] = value

        multiply(lhs, 0, lhs.shape[1], stored.at[j], tile, put)


def last_kernel(layout, count, rows, tile, base, ahead, cuts, plan, ids, copies_each, *refs):
    blocks, stored, parts, heads = refs[:count], refs[count], refs[count + 1 : count + 3], refs[count + 3 : count + 5]
    out_ref, lhs, policy_ref, reference_ref, fresh, sems = refs[count + 5 :]
    logits = (policy_ref, reference_ref)
    columns = policy_ref.shape[1]
    copies = copies_of(cuts, plan, heads, [fresh.at[0], fresh.at[1]], sems, ahead)
    for copy in copies:
        copy.start()
    fill(layout, blocks, rows, lhs)
    if ahead:
        for j, (part, logit) in enumerate(zip(parts, logits)):

            def put(at, value):
                logit[:, at] = part[:, at] + value

            multiply(lhs, 0, ahead, stored.at[j, pl.ds(base, ahead)], tile, put)
    groups = 1 if ahead else 2
    size = -(-len(cuts) // groups)
    for i in range(0, len(cuts), size):
        low, high = cuts[i][0], cuts[i + size][0] if i + size < len(cuts) else lhs.shape[1]
        for j, (part, logit) in enumerate(zip(parts, logits)):
            for copy in copies[2 * i + j : 2 * (i + size) : 2]:
                copy.wait()

            def more(at, value):
                logit[:, at] = (logit if low else part)[:, at] + value

            multiply(lhs, low, high, fresh.at[j, pl.ds(low - ahead, high - low)], tile, more)

    digits = jnp.concatenate([blocks[i][row : row + rows, column : column + LANES] for i, row, column in ids], axis=0)
    digits = digits.astype(jnp.float32)
    ids = digits[:, 0:1] + digits[:, 1:2] * 256.0 + digits[:, 2:3] * 65536.0
    policy, reference = logits[0][...], logits[1][...]
    base = ((lax.axis_index("tok") * lax.axis_size("vocab") + lax.axis_index("vocab")) * columns).astype(jnp.float32)
    hits = lax.broadcasted_iota(jnp.int32, policy.shape, 1).astype(jnp.float32) == ids - base
    peak_policy = jnp.max(policy, axis=1, keepdims=True)
    peak_reference = jnp.max(reference, axis=1, keepdims=True)
    policy_exp = jnp.exp(policy - peak_policy)
    stats = (
        peak_policy,
        peak_reference,
        jnp.sum(policy_exp, axis=1, keepdims=True),
        jnp.sum(jnp.exp(reference - peak_reference), axis=1, keepdims=True),
        jnp.sum(policy_exp * (policy - reference), axis=1, keepdims=True),
        jnp.sum(jnp.where(hits, policy, 0.0), axis=1, keepdims=True),
        jnp.sum(jnp.where(hits, reference, 0.0), axis=1, keepdims=True),
    )
    lane = lax.broadcasted_iota(jnp.int32, (policy.shape[0], LANES), 1)
    table = jnp.zeros((policy.shape[0], LANES), jnp.float32)
    for s, stat in enumerate(stats):
        table = jnp.where(lane == s, stat, table)
    turned = table.T
    me = lax.axis_index("tok")
    for b in range(policy.shape[0] // rows):
        line = jnp.concatenate([turned[s : s + 1, b * rows : (b + 1) * rows] for s in range(STATS)], axis=1)
        spare = out_ref.shape[2] - STATS * rows
        line = jnp.concatenate([line, jnp.zeros((1, spare), jnp.float32)], axis=1)
        for j in range(copies_each):
            out_ref[(me ^ b) * copies_each + j] = line


def finish_kernel(rows, got_ref, policy_ref, reference_ref, divergence_ref):
    got = got_ref[...][:, 0, :]
    stat = [got[:, s * rows : (s + 1) * rows] for s in range(STATS)]
    peak_policy = jnp.max(stat[0], axis=0, keepdims=True)
    peak_reference = jnp.max(stat[1], axis=0, keepdims=True)
    policy_scale = jnp.exp(stat[0] - peak_policy)
    reference_scale = jnp.exp(stat[1] - peak_reference)
    total_policy = jnp.sum(stat[2] * policy_scale, axis=0, keepdims=True)
    total_reference = jnp.sum(stat[3] * reference_scale, axis=0, keepdims=True)
    weighted = jnp.sum(stat[4] * policy_scale, axis=0, keepdims=True)
    log_norm_policy = peak_policy + jnp.log(total_policy)
    log_norm_reference = peak_reference + jnp.log(total_reference)
    policy_ref[...] = jnp.sum(stat[5], axis=0, keepdims=True) - log_norm_policy
    reference_ref[...] = jnp.sum(stat[6], axis=0, keepdims=True) - log_norm_reference
    divergence_ref[...] = weighted / total_policy - log_norm_policy + log_norm_reference


def in_vmem(value):
    return pltpu.with_memory_space_constraint(value, pltpu.VMEM)


def layout_of(pieces, spans):
    arrays, layout, to = [], [], 0
    for m, column, width, _ in spans:
        for array, row, block in pieces[m]:
            index = next((i for i, seen in enumerate(arrays) if seen is array), len(arrays))
            if index == len(arrays):
                arrays.append(array)
            layout.append((index, row, column, width, block, to))
        to += width
    return arrays, layout, to


def body(hidden, policy_head, reference_head, targets):
    tok_count = lax.axis_size("tok")
    vocab_count = lax.axis_size("vocab")
    rows, depth = hidden.shape
    columns = policy_head.shape[1]
    tokens = rows * tok_count
    plan = Plan(depth, vocab_count)
    pieces = gather_rows(hidden, targets, plan, tok_count, vocab_count)
    vmem, hbm = (pl.BlockSpec(memory_space=space) for space in (pltpu.VMEM, pltpu.HBM))
    heads = [pltpu.with_memory_space_constraint(head, pltpu.HBM) for head in (policy_head, reference_head)]
    tile = min(TILE, columns)
    kind = policy_head.dtype
    bytes_of = lambda *shape: 2 * functools.reduce(lambda a, b: a * b, shape)

    def prepared(near):
        spans = plan.spans(near)
        return chunked(spans), *layout_of(pieces, spans)

    def cost(width, exps=0):
        return pl.CostEstimate(flops=4 * tokens * columns * width, bytes_accessed=0, transcendentals=exps)

    cuts, arrays, layout, width = prepared(True)
    far_cuts, far_arrays, far_layout, far_width = prepared(False)
    ahead = max([at + part for at, _, _, part in far_cuts if at + part <= AHEAD] or [0])
    soon = [(width + cut[0], *cut[1:]) for cut in far_cuts if cut[0] < ahead]
    later = [cut for cut in far_cuts if cut[0] >= ahead]
    left = far_width - ahead
    limit = pltpu.CompilerParams(
        vmem_limit_bytes=MARGIN + bytes_of(tokens, far_width) + bytes_of(4, tokens, columns) + bytes_of(2, left, columns)
    )
    stored = pl.pallas_call(
        functools.partial(load_kernel, cuts + soon, plan),
        out_shape=pltpu.VMEM((2, width + ahead, columns), kind),
        in_specs=[hbm] * 2,
        out_specs=vmem,
        scratch_shapes=[pltpu.SemaphoreType.DMA((len(cuts + soon), 2))],
        compiler_params=limit,
        cost_estimate=cost(width),
        name="load_first",
    )(*heads)

    parts = pl.pallas_call(
        functools.partial(partial_kernel, layout, len(arrays), rows, tile),
        out_shape=[pltpu.VMEM((tokens, columns), jnp.float32)] * 2,
        in_specs=[vmem] * (len(arrays) + 1),
        out_specs=[vmem] * 2,
        scratch_shapes=[pltpu.VMEM((tokens, width), kind)],
        compiler_params=limit,
        cost_estimate=cost(width),
        name="first_part",
    )(*[in_vmem(a) for a in arrays], in_vmem(stored))

    ids = {}
    for array, row, block in pieces[0]:
        index = next((i for i, seen in enumerate(far_arrays) if seen is array), len(far_arrays))
        if index == len(far_arrays):
            far_arrays.append(array)
        ids[block] = (index, row, plan.wide + plan.both)
    span = -(-STATS * rows // LANES) * LANES
    packed = pl.pallas_call(
        functools.partial(
            last_kernel, far_layout, len(far_arrays), rows, tile, width, ahead, later, plan,
            [ids[b] for b in range(tok_count)], vocab_count,
        ),
        out_shape=jax.ShapeDtypeStruct((tok_count * vocab_count, 1, span), jnp.float32),
        in_specs=[vmem] * (len(far_arrays) + 3) + [hbm] * 2,
        out_specs=vmem,
        scratch_shapes=[
            pltpu.VMEM((tokens, far_width), kind),
            pltpu.VMEM((tokens, columns), jnp.float32),
            pltpu.VMEM((tokens, columns), jnp.float32),
            pltpu.VMEM((2, left, columns), kind),
            pltpu.SemaphoreType.DMA((len(later), 2)),
        ],
        compiler_params=limit,
        cost_estimate=cost(far_width, 2 * tokens * columns),
        name="last_part",
    )(
        *[in_vmem(a) for a in far_arrays],
        in_vmem(stored),
        *[in_vmem(p) for p in parts],
        *heads,
    )

    got = lax.all_to_all(packed, ("tok", "vocab"), split_axis=0, concat_axis=0, tiled=True)
    outs = pl.pallas_call(
        functools.partial(finish_kernel, rows),
        out_shape=[jax.ShapeDtypeStruct((1, rows), jnp.float32)] * 3,
        in_specs=[vmem],
        out_specs=[vmem] * 3,
        name="finish",
    )(got)
    return tuple(out.reshape(rows) for out in outs)


def solution(mesh):
    in_specs = (P("tok", None), P(None, ("tok", "vocab")), P(None, ("tok", "vocab")), P("tok"))
    out_specs = (P("tok"), P("tok"), P("tok"))

    return jax.shard_map(body, mesh=mesh, in_specs=in_specs, out_specs=out_specs, check_vma=False)
```

```python
import functools

import jax
import jax.numpy as jnp
from jax import lax
from jax.experimental import pallas as pl
from jax.experimental.pallas import tpu as pltpu
from jax.sharding import PartitionSpec as P


LANES = 128
TILE = 512
CHUNK = 768
STATS = 7
SPLIT = 9216
AHEAD = 2304
LOADS = (3072,)
MARGIN = 4 << 20


def hop(value, mask, count):
    pairs = [(i, i ^ mask) for i in range(count)]
    return lax.ppermute(value, ("tok", "vocab"), pairs)


def own_kernel(plan, edges, hidden_ref, targets_ref, out_ref, targets_vmem, sems):
    me = lax.axis_index("vocab")
    fetch = pltpu.make_async_copy(targets_ref, targets_vmem, sems.at[2 * plan.vocab_count])
    fetch.start()
    copies = []
    for m in range(plan.vocab_count):
        for kind, (to, width) in enumerate(((0, plan.wide), (plan.wide, plan.both if m < 2 else 0))):
            if width:
                start = pl.multiple_of(plan.starts(me ^ m)[kind], LANES)
                copies.append(
                    pltpu.make_async_copy(
                        hidden_ref.at[:, pl.ds(start, width)], out_ref.at[:, pl.ds(edges[m] + to, width)], sems.at[len(copies)]
                    )
                )
    for copy in copies:
        copy.start()
    rows = hidden_ref.shape[0]
    fetch.wait()
    spread = jnp.broadcast_to(targets_vmem[...].astype(jnp.float32), (rows, rows))
    here = lax.broadcasted_iota(jnp.int32, (rows, rows), 0) == lax.broadcasted_iota(jnp.int32, (rows, rows), 1)
    ids = jnp.sum(jnp.where(here, spread, 0.0), axis=1, keepdims=True).astype(jnp.int32)
    lane = lax.broadcasted_iota(jnp.int32, (rows, LANES), 1)
    digits = jnp.where(lane < 3, (ids >> (8 * jnp.minimum(lane, 3))) & 255, 0)
    out_ref[:, edges[1] - LANES : edges[1]] = digits.astype(jnp.float32).astype(out_ref.dtype)
    for copy in copies:
        copy.wait()


def own_columns(hidden, targets, plan):
    rows, kind = hidden.shape[0], hidden.dtype
    widths = [plan.wide + (plan.both if m < 2 else 0) + (LANES if m == 0 else 0) for m in range(plan.vocab_count)]
    edges = [sum(widths[:m]) for m in range(plan.vocab_count + 1)]
    vmem, hbm = (pl.BlockSpec(memory_space=space) for space in (pltpu.VMEM, pltpu.HBM))
    ordered = pl.pallas_call(
        functools.partial(own_kernel, plan, edges),
        out_shape=jax.ShapeDtypeStruct((rows, edges[-1]), kind),
        in_specs=[hbm] * 2,
        out_specs=vmem,
        scratch_shapes=[pltpu.VMEM((1, rows), targets.dtype), pltpu.SemaphoreType.DMA((2 * plan.vocab_count + 1,))],
        compiler_params=pltpu.CompilerParams(vmem_limit_bytes=MARGIN),
        name="own_columns",
    )(*[pltpu.with_memory_space_constraint(value, pltpu.HBM) for value in (hidden, targets.reshape(1, rows))])
    return [ordered[:, low:high] for low, high in zip(edges, edges[1:])]


class Plan:
    def __init__(self, depth, vocab_count):
        unit = vocab_count * LANES
        self.wide = min(SPLIT, depth) // unit * unit // vocab_count
        self.rest = depth - self.wide * vocab_count
        self.both = self.rest // 2
        self.vocab_count = vocab_count

    def starts(self, v):
        return v * self.wide, self.wide * self.vocab_count + (v & 1) * self.both

    def spans(self, near):
        found = []
        for m in range(self.vocab_count):
            if (m < 2) == near:
                found.append((m, 0, self.wide, 0))
                if m < 2 and self.both:
                    found.append((m, self.wide, self.both, 1))
        return found


def sends(tok_count):
    if tok_count == 8:
        return [[1, 2], [4], [6, 3, 5], [7]]
    return [list(range(1, tok_count))]


def turns(tok_count):
    if tok_count == 8:
        return [[1, 2, 4, 3], [6, 5, 7]]
    return [list(range(1, tok_count))]


def gather_rows(hidden, targets, plan, tok_count, vocab_count):
    rows = hidden.shape[0]

    def move(value, mask):
        return hop(value, mask, tok_count * vocab_count)

    own = own_columns(hidden, targets, plan)
    first = own[0]
    along, across = {0: first}, {}
    step = tok_count // 4
    while step >= 1:
        along.update({k ^ step: move(along[k], step * 2 * vocab_count) for k in list(along)})
        step //= 2
    for k in along:
        across[k] = move(along[k], vocab_count)
    blocks = {2 * k: along[k] for k in along} | {2 * k + 1: across[k] for k in across}
    pieces = {0: [(blocks[b], 0, b) for b in blocks]}

    def joined(names, width):
        return jnp.concatenate(lax.optimization_barrier([blocks[b][:, :width] for b in names]), axis=0)

    for m in range(vocab_count):
        if m % 2:
            continue
        if m:
            pieces[m] = [(own[m], 0, 0)]
            for names in sends(tok_count):
                got = move(joined(names, plan.wide), m)
                pieces[m] += [(got, i * rows, b) for i, b in enumerate(names)]
        pieces[m + 1] = [(own[m + 1], 0, 0)]
        if m == 0:
            groups = [(joined(names, plan.wide + plan.both), [(i * rows, b) for i, b in enumerate(names)]) for names in turns(tok_count)]
        else:
            seen = {}
            for array, at, b in pieces[m][1:]:
                seen.setdefault(id(array), (array, []))[1].append((at, b))
            groups = list(seen.values())
        for array, places in groups:
            got = move(array, 1)
            pieces[m + 1] += [(got, at, b) for at, b in places]
    return pieces


def chunked(spans):
    found, at = [], 0
    for m, _, width, kind in spans:
        for cut in range(0, width, CHUNK):
            part = min(CHUNK, width - cut)
            found.append((at, (m, kind), cut, part))
            at += part
    return found


def copies_of(cut_spans, plan, heads, stores, sems, low):
    found = []
    me = lax.axis_index("vocab")
    for i, (at, key, cut, part) in enumerate(cut_spans):
        for j, (head, store) in enumerate(zip(heads, stores)):
            start = plan.starts(me ^ key[0])[key[1]]
            src = pl.ds(pl.multiple_of(start, LANES) + cut, part)
            found.append(pltpu.make_async_copy(head.at[src, :], store.at[pl.ds(at - low, part), :], sems.at[i, j]))
    return found


def load_kernel(cuts, plan, policy_ref, reference_ref, *refs):
    stored, sems = refs[-2:]
    copies = copies_of(cuts, plan, (policy_ref, reference_ref), [stored.at[0], stored.at[1]], sems, 0)
    for copy in copies:
        copy.start()
    for copy in copies:
        copy.wait()


def fill(layout, refs, rows, lhs):
    for index, row, column, width, block, to in layout:
        lhs[block * rows : (block + 1) * rows, to : to + width] = refs[index][row : row + rows, column : column + width]


def multiply(lhs, low, high, store, tile, put):
    @pl.loop(0, store.shape[1] // tile)
    def _(step):
        at = pl.ds(pl.multiple_of(step * tile, tile), tile)
        put(at, jnp.dot(lhs[:, low:high], store[0 : high - low, at], preferred_element_type=jnp.float32))


def partial_kernel(layout, count, rows, tile, cuts, plan, *refs):
    heads, blocks, outs = refs[1:3], refs[3 : count + 3], refs[count + 3 : count + 5]
    stored, lhs, sems = refs[count + 5 :]
    copies = copies_of(cuts, plan, heads, [stored.at[0], stored.at[1]], sems, 0)
    for copy in copies:
        copy.start()
    fill(layout, blocks, rows, lhs)
    width = lhs.shape[1]
    for j, out in enumerate(outs):

        def put(at, value):
            out[:, at] = value

        multiply(lhs, 0, width, stored.at[j, pl.ds(0, width)], tile, put)
    for copy in copies:
        copy.wait()


def last_kernel(layout, count, rows, tile, base, ahead, cuts, plan, ids, copies_each, *refs):
    blocks, stored, parts, heads = refs[:count], refs[count], refs[count + 1 : count + 3], refs[count + 3 : count + 5]
    out_ref, lhs, policy_ref, reference_ref, fresh, sems = refs[count + 5 :]
    logits = (policy_ref, reference_ref)
    columns = policy_ref.shape[1]
    copies = copies_of(cuts, plan, heads, [fresh.at[0], fresh.at[1]], sems, ahead)
    for copy in copies[0::2] + copies[1::2]:
        copy.start()
    fill(layout, blocks, rows, lhs)
    if ahead:
        for j, (part, logit) in enumerate(zip(parts, logits)):

            def put(at, value):
                logit[:, at] = part[:, at] + value

            multiply(lhs, 0, ahead, stored.at[j, pl.ds(base, ahead)], tile, put)
    groups = 1 if ahead else 2
    size = -(-len(cuts) // groups)
    for i in range(0, len(cuts), size):
        low, high = cuts[i][0], cuts[i + size][0] if i + size < len(cuts) else lhs.shape[1]
        for j, (part, logit) in enumerate(zip(parts, logits)):
            for copy in copies[2 * i + j : 2 * (i + size) : 2]:
                copy.wait()

            def more(at, value):
                logit[:, at] = (logit if low else part)[:, at] + value

            multiply(lhs, low, high, fresh.at[j, pl.ds(low - ahead, high - low)], tile, more)

    digits = jnp.concatenate([blocks[i][row : row + rows, column : column + LANES] for i, row, column in ids], axis=0)
    digits = digits.astype(jnp.float32)
    ids = digits[:, 0:1] + digits[:, 1:2] * 256.0 + digits[:, 2:3] * 65536.0
    policy, reference = logits[0][...], logits[1][...]
    base = ((lax.axis_index("tok") * lax.axis_size("vocab") + lax.axis_index("vocab")) * columns).astype(jnp.float32)
    hits = lax.broadcasted_iota(jnp.int32, policy.shape, 1).astype(jnp.float32) == ids - base
    peak_policy = jnp.max(policy, axis=1, keepdims=True)
    peak_reference = jnp.max(reference, axis=1, keepdims=True)
    policy_exp = jnp.exp(policy - peak_policy)
    stats = (
        peak_policy,
        peak_reference,
        jnp.sum(policy_exp, axis=1, keepdims=True),
        jnp.sum(jnp.exp(reference - peak_reference), axis=1, keepdims=True),
        jnp.sum(policy_exp * (policy - reference), axis=1, keepdims=True),
        jnp.sum(jnp.where(hits, policy, 0.0), axis=1, keepdims=True),
        jnp.sum(jnp.where(hits, reference, 0.0), axis=1, keepdims=True),
    )
    lane = lax.broadcasted_iota(jnp.int32, (policy.shape[0], LANES), 1)
    table = jnp.zeros((policy.shape[0], LANES), jnp.float32)
    for s, stat in enumerate(stats):
        table = jnp.where(lane == s, stat, table)
    turned = table.T
    me = lax.axis_index("tok")
    for b in range(policy.shape[0] // rows):
        line = jnp.concatenate([turned[s : s + 1, b * rows : (b + 1) * rows] for s in range(STATS)], axis=1)
        spare = out_ref.shape[2] - STATS * rows
        line = jnp.concatenate([line, jnp.zeros((1, spare), jnp.float32)], axis=1)
        for j in range(copies_each):
            out_ref[(me ^ b) * copies_each + j] = line


def finish_kernel(rows, got_ref, policy_ref, reference_ref, divergence_ref):
    got = got_ref[...][:, 0, :]
    stat = [got[:, s * rows : (s + 1) * rows] for s in range(STATS)]
    peak_policy = jnp.max(stat[0], axis=0, keepdims=True)
    peak_reference = jnp.max(stat[1], axis=0, keepdims=True)
    policy_scale = jnp.exp(stat[0] - peak_policy)
    reference_scale = jnp.exp(stat[1] - peak_reference)
    total_policy = jnp.sum(stat[2] * policy_scale, axis=0, keepdims=True)
    total_reference = jnp.sum(stat[3] * reference_scale, axis=0, keepdims=True)
    weighted = jnp.sum(stat[4] * policy_scale, axis=0, keepdims=True)
    log_norm_policy = peak_policy + jnp.log(total_policy)
    log_norm_reference = peak_reference + jnp.log(total_reference)
    policy_ref[...] = jnp.sum(stat[5], axis=0, keepdims=True) - log_norm_policy
    reference_ref[...] = jnp.sum(stat[6], axis=0, keepdims=True) - log_norm_reference
    divergence_ref[...] = weighted / total_policy - log_norm_policy + log_norm_reference


def in_vmem(value):
    return pltpu.with_memory_space_constraint(value, pltpu.VMEM)


def layout_of(pieces, spans):
    arrays, layout, to = [], [], 0
    for m, column, width, _ in spans:
        for array, row, block in pieces[m]:
            index = next((i for i, seen in enumerate(arrays) if seen is array), len(arrays))
            if index == len(arrays):
                arrays.append(array)
            layout.append((index, row, column, width, block, to))
        to += width
    return arrays, layout, to


def body(hidden, policy_head, reference_head, targets):
    tok_count = lax.axis_size("tok")
    vocab_count = lax.axis_size("vocab")
    rows, depth = hidden.shape
    columns = policy_head.shape[1]
    tokens = rows * tok_count
    plan = Plan(depth, vocab_count)
    pieces = gather_rows(hidden, targets, plan, tok_count, vocab_count)
    vmem, hbm = (pl.BlockSpec(memory_space=space) for space in (pltpu.VMEM, pltpu.HBM))
    heads = [pltpu.with_memory_space_constraint(head, pltpu.HBM) for head in (policy_head, reference_head)]
    tile = min(TILE, columns)
    kind = policy_head.dtype
    bytes_of = lambda *shape: 2 * functools.reduce(lambda a, b: a * b, shape)

    def prepared(near):
        spans = plan.spans(near)
        return chunked(spans), *layout_of(pieces, spans)

    def cost(width, exps=0):
        return pl.CostEstimate(flops=4 * tokens * columns * width, bytes_accessed=0, transcendentals=exps)

    cuts, arrays, layout, width = prepared(True)
    far_cuts, far_arrays, far_layout, far_width = prepared(False)
    ahead = max([at + part for at, _, _, part in far_cuts if at + part <= AHEAD] or [0])
    soon = [(width + cut[0], *cut[1:]) for cut in far_cuts if cut[0] < ahead]
    later = [cut for cut in far_cuts if cut[0] >= ahead]
    left = far_width - ahead
    limit = pltpu.CompilerParams(
        vmem_limit_bytes=MARGIN + bytes_of(tokens, far_width) + bytes_of(4, tokens, columns) + bytes_of(2, left, columns)
    )
    store = pltpu.VMEM((2, width + ahead, columns), kind)
    limits = [at for at in LOADS if at < width] + [width]
    stored = None
    for i, (low, high) in enumerate(zip([0] + limits, limits)):
        part = [cut for cut in cuts if low <= cut[0] < high]
        stored = pl.pallas_call(
            functools.partial(load_kernel, part, plan),
            out_shape=store,
            in_specs=[hbm] * 2 + [vmem] * (i > 0),
            out_specs=vmem,
            scratch_shapes=[pltpu.SemaphoreType.DMA((len(part), 2))],
            input_output_aliases={2: 0} if i else {},
            compiler_params=limit,
            cost_estimate=cost(high - low),
            name="load_heads",
        )(*heads, *([in_vmem(stored)] if i else []))

    *parts, stored = pl.pallas_call(
        functools.partial(partial_kernel, layout, len(arrays), rows, tile, soon, plan),
        out_shape=[pltpu.VMEM((tokens, columns), jnp.float32)] * 2 + [store],
        in_specs=[vmem] + [hbm] * 2 + [vmem] * len(arrays),
        out_specs=[vmem] * 3,
        scratch_shapes=[pltpu.VMEM((tokens, width), kind), pltpu.SemaphoreType.DMA((len(soon) or 1, 2))],
        input_output_aliases={0: 2},
        compiler_params=limit,
        cost_estimate=cost(width),
        name="first_part",
    )(in_vmem(stored), *heads, *[in_vmem(a) for a in arrays])

    ids = {}
    for array, row, block in pieces[0]:
        index = next((i for i, seen in enumerate(far_arrays) if seen is array), len(far_arrays))
        if index == len(far_arrays):
            far_arrays.append(array)
        ids[block] = (index, row, plan.wide + plan.both)
    span = -(-STATS * rows // LANES) * LANES
    packed = pl.pallas_call(
        functools.partial(
            last_kernel, far_layout, len(far_arrays), rows, tile, width, ahead, later, plan,
            [ids[b] for b in range(tok_count)], vocab_count,
        ),
        out_shape=jax.ShapeDtypeStruct((tok_count * vocab_count, 1, span), jnp.float32),
        in_specs=[vmem] * (len(far_arrays) + 3) + [hbm] * 2,
        out_specs=vmem,
        scratch_shapes=[
            pltpu.VMEM((tokens, far_width), kind),
            pltpu.VMEM((tokens, columns), jnp.float32),
            pltpu.VMEM((tokens, columns), jnp.float32),
            pltpu.VMEM((2, left, columns), kind),
            pltpu.SemaphoreType.DMA((len(later), 2)),
        ],
        compiler_params=limit,
        cost_estimate=cost(far_width, 2 * tokens * columns),
        name="last_part",
    )(
        *[in_vmem(a) for a in far_arrays],
        in_vmem(stored),
        *[in_vmem(p) for p in parts],
        *heads,
    )

    got = lax.all_to_all(packed, ("tok", "vocab"), split_axis=0, concat_axis=0, tiled=True)
    outs = pl.pallas_call(
        functools.partial(finish_kernel, rows),
        out_shape=[jax.ShapeDtypeStruct((1, rows), jnp.float32)] * 3,
        in_specs=[vmem],
        out_specs=[vmem] * 3,
        name="finish",
    )(in_vmem(got))
    return tuple(out.reshape(rows) for out in outs)


def solution(mesh):
    in_specs = (P("tok", None), P(None, ("tok", "vocab")), P(None, ("tok", "vocab")), P("tok"))
    out_specs = (P("tok"), P("tok"), P("tok"))

    return jax.shard_map(body, mesh=mesh, in_specs=in_specs, out_specs=out_specs, check_vma=False)
```

```python
import functools

import jax
import jax.numpy as jnp
from jax import lax
from jax.experimental import pallas as pl
from jax.experimental.pallas import tpu as pltpu
from jax.sharding import PartitionSpec as P


LANES = 128
TILE = 1024
CHUNK = 768
STATS = 7
SPLIT = 9216
AHEAD = 768
LOADS = (2304, 3840)
MARGIN = 4 << 20
FLOOR = 16 << 20


def hop(value, mask, count):
    pairs = [(i, i ^ mask) for i in range(count)]
    return lax.ppermute(value, ("tok", "vocab"), pairs)


def own_kernel(plan, edges, hidden_ref, targets_ref, out_ref, targets_vmem, sems):
    me = lax.axis_index("vocab")
    fetch = pltpu.make_async_copy(targets_ref, targets_vmem, sems.at[2 * plan.vocab_count])
    fetch.start()
    copies = []
    for m in range(plan.vocab_count):
        for kind, (to, width) in enumerate(((0, plan.wide), (plan.wide, plan.both if m < 2 else 0))):
            if width:
                start = pl.multiple_of(plan.starts(me ^ m)[kind], LANES)
                copies.append(
                    pltpu.make_async_copy(
                        hidden_ref.at[:, pl.ds(start, width)], out_ref.at[:, pl.ds(edges[m] + to, width)], sems.at[len(copies)]
                    )
                )
    for copy in copies:
        copy.start()
    rows = hidden_ref.shape[0]
    fetch.wait()
    spread = jnp.broadcast_to(targets_vmem[...].astype(jnp.float32), (rows, rows))
    here = lax.broadcasted_iota(jnp.int32, (rows, rows), 0) == lax.broadcasted_iota(jnp.int32, (rows, rows), 1)
    ids = jnp.sum(jnp.where(here, spread, 0.0), axis=1, keepdims=True).astype(jnp.int32)
    lane = lax.broadcasted_iota(jnp.int32, (rows, LANES), 1)
    digits = jnp.where(lane < 3, (ids >> (8 * jnp.minimum(lane, 3))) & 255, 0)
    out_ref[:, edges[1] - LANES : edges[1]] = digits.astype(jnp.float32).astype(out_ref.dtype)
    for copy in copies:
        copy.wait()


def own_columns(hidden, targets, plan):
    rows, kind = hidden.shape[0], hidden.dtype
    widths = [plan.wide + (plan.both if m < 2 else 0) + (LANES if m == 0 else 0) for m in range(plan.vocab_count)]
    edges = [sum(widths[:m]) for m in range(plan.vocab_count + 1)]
    vmem, hbm = (pl.BlockSpec(memory_space=space) for space in (pltpu.VMEM, pltpu.HBM))
    ordered = pl.pallas_call(
        functools.partial(own_kernel, plan, edges),
        out_shape=jax.ShapeDtypeStruct((rows, edges[-1]), kind),
        in_specs=[hbm] * 2,
        out_specs=vmem,
        scratch_shapes=[pltpu.VMEM((1, rows), targets.dtype), pltpu.SemaphoreType.DMA((2 * plan.vocab_count + 1,))],
        compiler_params=pltpu.CompilerParams(vmem_limit_bytes=MARGIN),
        name="own_columns",
    )(*[pltpu.with_memory_space_constraint(value, pltpu.HBM) for value in (hidden, targets.reshape(1, rows))])
    return [ordered[:, low:high] for low, high in zip(edges, edges[1:])]


class Plan:
    def __init__(self, depth, vocab_count):
        unit = vocab_count * LANES
        self.wide = min(SPLIT, depth) // unit * unit // vocab_count
        self.rest = depth - self.wide * vocab_count
        self.both = self.rest // 2
        self.vocab_count = vocab_count

    def starts(self, v):
        return v * self.wide, self.wide * self.vocab_count + (v & 1) * self.both

    def spans(self, turn):
        found = []
        for m in range(self.vocab_count):
            if turn == (0 if m < 2 else 1 + m % 2):
                found.append((m, 0, self.wide, 0))
                if m < 2 and self.both:
                    found.append((m, self.wide, self.both, 1))
        return found


def sends(tok_count):
    if tok_count == 8:
        return [[1, 2], [4], [6, 3, 5], [7]]
    return [list(range(1, tok_count))]


def turns(tok_count):
    if tok_count == 8:
        return [[1, 2, 4, 3], [6, 5, 7]]
    return [list(range(1, tok_count))]


def gather_rows(hidden, targets, plan, tok_count, vocab_count):
    rows = hidden.shape[0]

    def move(value, mask):
        return hop(value, mask, tok_count * vocab_count)

    own = own_columns(hidden, targets, plan)
    first = own[0]
    along, across = {0: first}, {}
    step = tok_count // 4
    while step >= 1:
        along.update({k ^ step: move(along[k], step * 2 * vocab_count) for k in list(along)})
        step //= 2
    for k in along:
        across[k] = move(along[k], vocab_count)
    blocks = {2 * k: along[k] for k in along} | {2 * k + 1: across[k] for k in across}
    pieces = {0: [(blocks[b], 0, b) for b in blocks]}

    def joined(names, width):
        return jnp.concatenate(lax.optimization_barrier([blocks[b][:, :width] for b in names]), axis=0)

    for m in range(vocab_count):
        if m % 2:
            continue
        if m:
            pieces[m] = [(own[m], 0, 0)]
            for names in sends(tok_count):
                got = move(joined(names, plan.wide), m)
                pieces[m] += [(got, i * rows, b) for i, b in enumerate(names)]
        pieces[m + 1] = [(own[m + 1], 0, 0)]
        if m == 0:
            groups = [(joined(names, plan.wide + plan.both), [(i * rows, b) for i, b in enumerate(names)]) for names in turns(tok_count)]
        else:
            seen = {}
            for array, at, b in pieces[m][1:]:
                seen.setdefault(id(array), (array, []))[1].append((at, b))
            groups = list(seen.values())
        for array, places in groups:
            got = move(array, 1)
            pieces[m + 1] += [(got, at, b) for at, b in places]
    return pieces


def chunked(spans):
    found, at = [], 0
    for m, _, width, kind in spans:
        for cut in range(0, width, CHUNK):
            part = min(CHUNK, width - cut)
            found.append((at, (m, kind), cut, part))
            at += part
    return found


def copies_of(cut_spans, plan, heads, stores, sems, low):
    found = []
    me = lax.axis_index("vocab")
    for i, (at, key, cut, part) in enumerate(cut_spans):
        for j, (head, store) in enumerate(zip(heads, stores)):
            start = plan.starts(me ^ key[0])[key[1]]
            src = pl.ds(pl.multiple_of(start, LANES) + cut, part)
            found.append(pltpu.make_async_copy(head.at[src, :], store.at[pl.ds(at - low, part), :], sems.at[i, j]))
    return found


def load_kernel(cuts, plan, policy_ref, reference_ref, *refs):
    stored, sems = refs[-2:]
    copies = copies_of(cuts, plan, (policy_ref, reference_ref), [stored.at[0], stored.at[1]], sems, 0)
    for copy in copies:
        copy.start()
    for copy in copies:
        copy.wait()


def fill(layout, refs, rows, lhs):
    for index, row, column, width, block, to in layout:
        lhs[block * rows : (block + 1) * rows, to : to + width] = refs[index][row : row + rows, column : column + width]


def multiply(lhs, low, high, store, tile, put):
    @pl.loop(0, store.shape[1] // tile)
    def _(step):
        at = pl.ds(pl.multiple_of(step * tile, tile), tile)
        put(at, jnp.dot(lhs[:, low:high], store[0 : high - low, at], preferred_element_type=jnp.float32))


def run_copies(cuts, plan, heads, stored, sems):
    copies = copies_of(cuts, plan, heads, [stored.at[0], stored.at[1]], sems, 0)
    for copy in copies:
        copy.start()
    return copies


def partial_kernel(layout, count, rows, tile, base, first, cuts, plan, *refs):
    heads, blocks = refs[1:3], refs[3 : count + 3]
    befores, (*outs, stored, lhs, sems) = refs[count + 3 : count + (3 if first else 5)], refs[count + (3 if first else 5) :]
    copies = run_copies(cuts, plan, heads, stored, sems)
    fill(layout, blocks, rows, lhs)
    width = lhs.shape[1]
    for j, out in enumerate(outs):

        def put(at, value):
            out[:, at] = value if first else befores[j][:, at] + value

        multiply(lhs, 0, width, stored.at[j, pl.ds(base, width)], tile, put)
    for copy in copies:
        copy.wait()


def last_kernel(layout, count, rows, tile, spots, ids, copies_each, *refs):
    blocks, stored, parts = refs[:count], refs[count], refs[count + 1 : count + 3]
    out_ref, lhs, policy_ref, reference_ref = refs[count + 3 :]
    logits = (policy_ref, reference_ref)
    columns = policy_ref.shape[1]
    fill(layout, blocks, rows, lhs)
    for j, (part, logit) in enumerate(zip(parts, logits)):

        @pl.loop(0, columns // tile)
        def _(step):
            at = pl.ds(pl.multiple_of(step * tile, tile), tile)
            total = part[:, at]
            for low, high, base in spots:
                if high > low:
                    weights = stored[j, base : base + high - low, at]
                    total += jnp.dot(lhs[:, low:high], weights, preferred_element_type=jnp.float32)
            logit[:, at] = total

    digits = jnp.concatenate([blocks[i][row : row + rows, column : column + LANES] for i, row, column in ids], axis=0)
    digits = digits.astype(jnp.float32)
    ids = digits[:, 0:1] + digits[:, 1:2] * 256.0 + digits[:, 2:3] * 65536.0
    policy, reference = logits[0][...], logits[1][...]
    base = ((lax.axis_index("tok") * lax.axis_size("vocab") + lax.axis_index("vocab")) * columns).astype(jnp.float32)
    hits = lax.broadcasted_iota(jnp.int32, policy.shape, 1).astype(jnp.float32) == ids - base
    peak_policy = jnp.max(policy, axis=1, keepdims=True)
    peak_reference = jnp.max(reference, axis=1, keepdims=True)
    policy_exp = jnp.exp(policy - peak_policy)
    stats = (
        peak_policy,
        peak_reference,
        jnp.sum(policy_exp, axis=1, keepdims=True),
        jnp.sum(jnp.exp(reference - peak_reference), axis=1, keepdims=True),
        jnp.sum(policy_exp * (policy - reference), axis=1, keepdims=True),
        jnp.sum(jnp.where(hits, policy, 0.0), axis=1, keepdims=True),
        jnp.sum(jnp.where(hits, reference, 0.0), axis=1, keepdims=True),
    )
    lane = lax.broadcasted_iota(jnp.int32, (policy.shape[0], LANES), 1)
    table = jnp.zeros((policy.shape[0], LANES), jnp.float32)
    for s, stat in enumerate(stats):
        table = jnp.where(lane == s, stat, table)
    turned = table.T
    me = lax.axis_index("tok")
    for b in range(policy.shape[0] // rows):
        line = jnp.concatenate([turned[s : s + 1, b * rows : (b + 1) * rows] for s in range(STATS)], axis=1)
        spare = out_ref.shape[2] - STATS * rows
        line = jnp.concatenate([line, jnp.zeros((1, spare), jnp.float32)], axis=1)
        for j in range(copies_each):
            out_ref[(me ^ b) * copies_each + j] = line


def finish_kernel(rows, got_ref, policy_ref, reference_ref, divergence_ref):
    got = got_ref[...][:, 0, :]
    stat = [got[:, s * rows : (s + 1) * rows] for s in range(STATS)]
    peak_policy = jnp.max(stat[0], axis=0, keepdims=True)
    peak_reference = jnp.max(stat[1], axis=0, keepdims=True)
    policy_scale = jnp.exp(stat[0] - peak_policy)
    reference_scale = jnp.exp(stat[1] - peak_reference)
    total_policy = jnp.sum(stat[2] * policy_scale, axis=0, keepdims=True)
    total_reference = jnp.sum(stat[3] * reference_scale, axis=0, keepdims=True)
    weighted = jnp.sum(stat[4] * policy_scale, axis=0, keepdims=True)
    log_norm_policy = peak_policy + jnp.log(total_policy)
    log_norm_reference = peak_reference + jnp.log(total_reference)
    policy_ref[...] = jnp.sum(stat[5], axis=0, keepdims=True) - log_norm_policy
    reference_ref[...] = jnp.sum(stat[6], axis=0, keepdims=True) - log_norm_reference
    divergence_ref[...] = weighted / total_policy - log_norm_policy + log_norm_reference


def in_vmem(value):
    return pltpu.with_memory_space_constraint(value, pltpu.VMEM)


def layout_of(pieces, spans):
    arrays, layout, to = [], [], 0
    for m, column, width, _ in spans:
        for array, row, block in pieces[m]:
            index = next((i for i, seen in enumerate(arrays) if seen is array), len(arrays))
            if index == len(arrays):
                arrays.append(array)
            layout.append((index, row, column, width, block, to))
        to += width
    return arrays, layout, to


def body(hidden, policy_head, reference_head, targets):
    tok_count = lax.axis_size("tok")
    vocab_count = lax.axis_size("vocab")
    rows, depth = hidden.shape
    columns = policy_head.shape[1]
    tokens = rows * tok_count
    plan = Plan(depth, vocab_count)
    pieces = gather_rows(hidden, targets, plan, tok_count, vocab_count)
    vmem, hbm = (pl.BlockSpec(memory_space=space) for space in (pltpu.VMEM, pltpu.HBM))
    heads = [pltpu.with_memory_space_constraint(head, pltpu.HBM) for head in (policy_head, reference_head)]
    tile = min(TILE, columns)
    kind = policy_head.dtype
    bytes_of = lambda *shape: 2 * functools.reduce(lambda a, b: a * b, shape)

    def prepared(turn):
        spans = plan.spans(turn)
        return chunked(spans), *layout_of(pieces, spans)

    def cost(width, exps=0):
        return pl.CostEstimate(flops=4 * tokens * columns * width, bytes_accessed=0, transcendentals=exps)

    def shifted(part, by):
        return [(cut[0] + by, *cut[1:]) for cut in part]

    cuts, arrays, layout, width = prepared(0)
    even_cuts, even_arrays, even_layout, even_width = prepared(1)
    odd_cuts, odd_arrays, odd_layout, odd_width = prepared(2)
    ahead = min([cut[0] for cut in odd_cuts if cut[0] >= max(AHEAD, odd_width - width)] or [odd_width])
    soon = shifted(even_cuts, width) + shifted([cut for cut in odd_cuts if cut[0] < ahead], width + even_width)
    later = shifted([cut for cut in odd_cuts if cut[0] >= ahead], -ahead)
    spots = [(0, ahead, width + even_width), (ahead, odd_width, 0)]
    limit = pltpu.CompilerParams(
        vmem_limit_bytes=max(FLOOR, MARGIN + bytes_of(tokens, max(width, even_width, odd_width)) + bytes_of(4, tokens, columns))
    )
    store = pltpu.VMEM((2, width + even_width + ahead, columns), kind)
    limits = [at for at in LOADS if at < width] + [width]
    stored = None
    for i, (low, high) in enumerate(zip([0] + limits, limits)):
        part = [cut for cut in cuts if low <= cut[0] < high]
        stored = pl.pallas_call(
            functools.partial(load_kernel, part, plan),
            out_shape=store,
            in_specs=[hbm] * 2 + [vmem] * (i > 0),
            out_specs=vmem,
            scratch_shapes=[pltpu.SemaphoreType.DMA((len(part), 2))],
            input_output_aliases={2: 0} if i else {},
            compiler_params=limit,
            cost_estimate=cost(high - low),
            name="load_heads",
        )(*heads, *([in_vmem(stored)] if i else []))

    parts = []
    for base, turn_cuts, turn_arrays, turn_layout, turn_width in (
        (0, soon, arrays, layout, width), (width, later, even_arrays, even_layout, even_width)
    ):
        *parts, stored = pl.pallas_call(
            functools.partial(partial_kernel, turn_layout, len(turn_arrays), rows, tile, base, not parts, turn_cuts, plan),
            out_shape=[pltpu.VMEM((tokens, columns), jnp.float32)] * 2 + [store],
            in_specs=[vmem] + [hbm] * 2 + [vmem] * (len(turn_arrays) + len(parts)),
            out_specs=[vmem] * 3,
            scratch_shapes=[pltpu.VMEM((tokens, turn_width), kind), pltpu.SemaphoreType.DMA((len(turn_cuts) or 1, 2))],
            input_output_aliases={0: 2},
            compiler_params=limit,
            cost_estimate=cost(turn_width),
        )(in_vmem(stored), *heads, *[in_vmem(a) for a in turn_arrays], *[in_vmem(p) for p in parts])

    ids = {}
    for array, row, block in pieces[0]:
        index = next((i for i, seen in enumerate(odd_arrays) if seen is array), len(odd_arrays))
        if index == len(odd_arrays):
            odd_arrays.append(array)
        ids[block] = (index, row, plan.wide + plan.both)
    span = -(-STATS * rows // LANES) * LANES
    packed = pl.pallas_call(
        functools.partial(
            last_kernel, odd_layout, len(odd_arrays), rows, tile, spots,
            [ids[b] for b in range(tok_count)], vocab_count,
        ),
        out_shape=jax.ShapeDtypeStruct((tok_count * vocab_count, 1, span), jnp.float32),
        in_specs=[vmem] * (len(odd_arrays) + 3),
        out_specs=vmem,
        scratch_shapes=[
            pltpu.VMEM((tokens, odd_width), kind),
            pltpu.VMEM((tokens, columns), jnp.float32),
            pltpu.VMEM((tokens, columns), jnp.float32),
        ],
        compiler_params=limit,
        cost_estimate=cost(odd_width, 2 * tokens * columns),
        name="last_part",
    )(*[in_vmem(a) for a in odd_arrays], in_vmem(stored), *[in_vmem(p) for p in parts])

    got = lax.all_to_all(packed, ("tok", "vocab"), split_axis=0, concat_axis=0, tiled=True)
    outs = pl.pallas_call(
        functools.partial(finish_kernel, rows),
        out_shape=[jax.ShapeDtypeStruct((1, rows), jnp.float32)] * 3,
        in_specs=[vmem],
        out_specs=[vmem] * 3,
        name="finish",
    )(in_vmem(got))
    return tuple(out.reshape(rows) for out in outs)


def solution(mesh):
    in_specs = (P("tok", None), P(None, ("tok", "vocab")), P(None, ("tok", "vocab")), P("tok"))
    out_specs = (P("tok"), P("tok"), P("tok"))

    return jax.shard_map(body, mesh=mesh, in_specs=in_specs, out_specs=out_specs, check_vma=False)
```
